256 devices in a mesh: gx: 8 (over x, core), gy: 4 (over y), gz: 8 (over z).
Axes of the slice: x: 4, y: 4, z: 8, core: 2. Of those that a mesh axis runs over, the one named last changes fastest.
Arguments:
- atom_feat: bfloat16 [262144, 128], P(('gx', 'gy', 'gz')), may hold values from -6 to 6
- atom_env: bfloat16 [262144, 9, 128], P(('gx', 'gy', 'gz')), may hold values from -6 to 6
- export_index: int32 [65536], P(('gx', 'gy', 'gz')), may hold values from 0 to 1023
- pair_vec: float32 [3, 524288], P(None, ('gx', 'gy', 'gz')), may hold values from -8 to 8
- pair_center: int32 [524288], P(('gx', 'gy', 'gz')), may hold values from 0 to 1023
- pair_owner: int32 [524288, 1], P(('gx', 'gy', 'gz')), may hold values from 0 to 31; in each aligned block of 2048 rows (0 to 2047, 2048 to 4095, ...) at most 96 rows name the same one
- pair_neigh: int32 [524288], P(('gx', 'gy', 'gz')), may hold values from 0 to 7935
- pair_count: int32 [256], P(('gx', 'gy', 'gz')), may hold values from 512 to 2048
- center_proj: bfloat16 [128, 512], replicated, may hold values from -0.375 to 0.375
- neighbour_proj: bfloat16 [128, 512], replicated, may hold values from -0.375 to 0.375
- radial_proj: bfloat16 [8, 512], replicated, may hold values from -4 to 4
- hidden_proj: bfloat16 [512, 512], replicated, may hold values from -0.25 to 0.25
- split_proj: bfloat16 [512, 384], replicated, may hold values from -0.5 to 0.5
- scalar_proj: bfloat16 [384, 512], replicated, may hold values from -0.3125 to 0.3125
- path_gain: float32 [3, 128], replicated, may hold values from 0.1 to 1.9
- energy_proj: float32 [512], replicated, may hold values from -0.5 to 0.5
Outputs:
- pair_latent: bfloat16 [524288, 512], P(('gx', 'gy', 'gz'))
- pair_vector: bfloat16 [3, 524288, 128], P(None, ('gx', 'gy', 'gz'))
- atom_energy: float32 [262144], P(('gx', 'gy', 'gz'))
The draws below stay inside these ranges and needn't reach their ends.
Inputs may be any that keep to these rules, and one draw needn't show every extreme that they name: `pair_owner`: among the pair slots of one device at most 96 name the same owner, a bound that some block reaches of them.
All inputs are finite; a program needn't handle non-finite values.
Results may differ from the reference program's by a relative error of at most 0.0062.
Values may be sent and summed in bfloat16 or wider, within the bound.
A program may use at most 128 MiB of HBM per device.

```python
import math
import jax
import jax.numpy as jnp
import numpy as np
from jax import lax

CHANNELS = 128
LATENT = 512
BASIS = 8
ATOMS_DEV = 1024
EXPORT = 256
PAIRS_DEV = 2048
CAPACITY = 96
ATOMS = 262144
PAIRS = 524288
TABLE = 7936
N_GX = 8
N_GY = 4
N_GZ = 8
DEVICES = 256


def set_ends(entries, key, smallest, top_value):
    extent = entries.shape
    spot = [jax.random.randint(jax.random.fold_in(key, axis), (), 0, extent[axis]) for axis in range(len(extent))]
    entries = entries.at[tuple(spot)].set(smallest)
    longest = extent.index(max(extent))
    spot[longest] = (spot[longest] + 1) % extent[longest]
    return entries.at[tuple(spot)].set(top_value)


def level_of(key, dims, cuts, smallest, largest):
    loudness = 1.0
    for position, parts in cuts:
        heights = jax.random.uniform(jax.random.fold_in(jax.random.fold_in(key, 6), position), (parts,), jnp.float32, smallest / len(cuts), largest / len(cuts))
        loudness = loudness * jnp.repeat(jnp.exp(heights), dims[position] // parts).reshape((-1,) + (1,) * (len(dims) - 1 - position))
    return loudness


def routed_block(stream_key, own, number, rows, count, top, limit, lean):
    order = jax.random.permutation(stream_key, count)
    crowded, usual = load_shares(count, rows * top, limit, lean, True), load_shares(count, rows * top, limit, lean, False)
    places = jnp.arange(count)

    def named(sizes, turn):
        used = int((sizes > 0).sum())
        fixed = max(1, used // 4)
        moved = fixed + (places - fixed + turn * (used - fixed)) % max(1, count - fixed)
        return jnp.zeros((count,), jnp.int32).at[order[jnp.where(places < fixed, places, moved)]].set(jnp.asarray(sizes, jnp.int32))

    sizes = jnp.where(number % 4 == 0, named(crowded, number // 4), named(usual, number - number // 4 - 1))
    mixed = jax.random.permutation(jax.random.fold_in(own, 3), count)
    donor, taker = mixed[0:count // 2 * 2:2], mixed[1:count // 2 * 2:2]
    margin = jnp.minimum(sizes[donor] - 1, limit - sizes[taker]) // 2
    margin = jnp.where((donor == order[0]) | (taker == order[0]) | (sizes[taker] == 0), 0, jnp.maximum(margin, 0))
    moved = jax.random.randint(jax.random.fold_in(own, 4), (count // 2,), 0, 1 << 20) % (margin + 1)
    sizes = sizes.at[donor].add(-moved).at[taker].add(moved)
    members = jnp.searchsorted(jnp.cumsum(sizes), jnp.arange(rows * top), side="right").astype(jnp.int32)
    table = members.reshape(top, rows).T
    table = table[jax.random.permutation(jax.random.fold_in(own, 1), rows)]
    turn = jax.random.randint(jax.random.fold_in(own, 2), (rows, 1), 0, top)
    return jnp.take_along_axis(table, (jnp.arange(top)[None, :] + turn) % top, axis=1)


def load_shares(number_of, total, most, lean, full):
    loads = [(1 << 20) // math.isqrt(rank ** lean) + 1 for rank in range(1, number_of + 1)]
    largest = most if full else min(most, max(-(-total // number_of), total * loads[0] // sum(loads)))
    least = 1 if total - largest >= number_of - 1 else 0
    given, surplus = [largest] + [least] * (number_of - 1), total - largest - least * (number_of - 1)
    while surplus > 0:
        movable = [i for i in range(1, number_of) if given[i] < largest] or [i for i in range(1, number_of) if given[i] < most]
        mass, budget = sum([loads[i] for i in movable]), surplus
        for i in movable:
            extra = min(most - given[i], max(1, budget * loads[i] // mass), surplus)
            given[i] = given[i] + extra
            surplus = surplus - extra
    return np.array(given)


def normal_values(own_key, shape, spread, reach, pieces=(), held_as=jnp.bfloat16):
    drawn = spread * jax.random.normal(own_key, shape, jnp.float32)
    if pieces:
        drawn = drawn * level_of(own_key, shape, pieces, -0.22, 0.18)
    return jnp.clip(drawn, -reach, reach).astype(held_as)


def setup_inputs(seed: int = 0) -> dict:
    splits = jax.random.split(jax.random.key(seed), 17)
    atom_feat = normal_values(splits[0], (ATOMS, CHANNELS), 1.0, 6.0, ((0, 256),))
    atom_env = normal_values(splits[1], (ATOMS, 9, CHANNELS), 1.0, 6.0, ((0, 256),))
    export_index = set_ends(jax.random.randint(splits[2], (DEVICES * EXPORT,), 0, ATOMS_DEV), jax.random.fold_in(splits[2], 1), 0, ATOMS_DEV - 1).astype(jnp.int32)
    pair_vec = normal_values(splits[3], (3, PAIRS), 2.0, 8.0, ((1, 256),), jnp.float32)
    pair_center = set_ends(jax.random.randint(splits[4], (PAIRS,), 0, ATOMS_DEV), jax.random.fold_in(splits[4], 1), 0, ATOMS_DEV - 1).astype(jnp.int32)
    pair_owner_keys = jax.random.split(jax.random.fold_in(splits[5], 1), PAIRS // PAIRS_DEV)
    pair_owner_turns = jax.random.permutation(jax.random.fold_in(splits[5], 3), PAIRS // PAIRS_DEV)
    pair_owner = jax.vmap(lambda own, number: routed_block(jax.random.fold_in(splits[5], 2), own, number, PAIRS_DEV, N_GY * N_GZ, 1, CAPACITY, 1))(pair_owner_keys, pair_owner_turns).reshape((PAIRS, 1))
    pair_neigh = set_ends(jax.random.randint(splits[6], (PAIRS,), 0, TABLE), jax.random.fold_in(splits[6], 1), 0, TABLE - 1).astype(jnp.int32)
    pair_count = set_ends(jax.random.randint(splits[7], (DEVICES,), PAIRS_DEV // 4, PAIRS_DEV + 1), jax.random.fold_in(splits[7], 1), PAIRS_DEV // 4, PAIRS_DEV).astype(jnp.int32)
    center_proj = normal_values(splits[8], (CHANNELS, LATENT), (2 * CHANNELS) ** -0.5, 0.375)
    neighbour_proj = normal_values(splits[9], (CHANNELS, LATENT), (2 * CHANNELS) ** -0.5, 0.375)
    radial_proj = normal_values(splits[10], (BASIS, LATENT), 2 ** -0.5, 4.0)
    hidden_proj = normal_values(splits[11], (LATENT, LATENT), LATENT ** -0.5, 0.25)
    split_proj = normal_values(splits[12], (LATENT, 3 * CHANNELS), (LATENT // 4) ** -0.5, 0.5)
    scalar_proj = normal_values(splits[13], (3 * CHANNELS, LATENT), (3 * CHANNELS) ** -0.5, 0.3125)
    path_gain = jnp.clip(1.0 + 0.18 * jax.random.normal(splits[14], (3, CHANNELS), jnp.float32), 0.1, 1.9)
    energy_proj = normal_values(splits[15], (LATENT,), (LATENT // 4) ** -0.5, 0.5, (), jnp.float32)
    return dict(atom_feat=atom_feat, atom_env=atom_env, export_index=export_index, pair_vec=pair_vec, pair_center=pair_center, pair_owner=pair_owner, pair_neigh=pair_neigh, pair_count=pair_count, center_proj=center_proj, neighbour_proj=neighbour_proj, radial_proj=radial_proj, hidden_proj=hidden_proj, split_proj=split_proj, scalar_proj=scalar_proj, path_gain=path_gain, energy_proj=energy_proj)


cutoff = 6.0
root_two = 2.0 ** 0.5
root_three = 3.0 ** 0.5
root_five = 5.0 ** 0.5
root_fifteen = 15.0 ** 0.5

def harmonics(unit):
    ux, uy, uz = (unit[0], unit[1], unit[2])
    first = root_three * unit
    second = jnp.stack([root_fifteen * ux * uy, root_fifteen * uy * uz, 0.5 * root_five * (2.0 * uz * uz - ux * ux - uy * uy), root_fifteen * ux * uz, 0.5 * root_fifteen * (ux * ux - uy * uy)])
    return (first, second)

def pair_block(h_center, env_center, h_neighbour, geometry, live, center_proj, neighbour_proj, radial_proj, hidden_proj, split_proj, scalar_proj, path_gain, energy_proj):
    channels = h_center.shape[1]
    basis = radial_proj.shape[0]
    length = jnp.sqrt(lax.optimization_barrier(jnp.sum(geometry * geometry, axis=0)))
    unit = geometry / jnp.maximum(length, 1.0)[None, :]
    spacing = cutoff / (basis - 1)
    centres = jnp.arange(basis).astype(geometry.dtype) * spacing
    radial = jnp.exp(-jnp.square((length[:, None] - centres[None, :]) / spacing))
    before = jnp.dot(h_center, center_proj, preferred_element_type=jnp.float32)
    before = before + jnp.dot(h_neighbour, neighbour_proj, preferred_element_type=jnp.float32)
    before = before + jnp.dot(radial, radial_proj.astype(jnp.float32), precision=lax.Precision.HIGHEST)
    hidden = jax.nn.silu(before).astype(jnp.bfloat16)
    latent = jax.nn.silu(jnp.dot(hidden, hidden_proj, preferred_element_type=jnp.float32)).astype(jnp.bfloat16)
    mixed = jnp.dot(latent, split_proj, preferred_element_type=jnp.float32)
    scalar_part = mixed[:, :channels]
    vector_part = mixed[:, channels:2 * channels]
    tensor_part = mixed[:, 2 * channels:]
    first, second = harmonics(unit)
    envelope = env_center.astype(jnp.float32)
    env_scalar = envelope[:, 0, :]
    env_vector = jnp.moveaxis(envelope[:, 1:4, :], 1, 0)
    env_tensor = jnp.moveaxis(envelope[:, 4:9, :], 1, 0)
    edge_vector = vector_part[None] * first[:, :, None]
    edge_tensor = tensor_part[None] * second[:, :, None]
    invariants = jnp.concatenate([scalar_part * env_scalar, lax.optimization_barrier(jnp.sum(edge_vector * env_vector, axis=0)) / root_three, lax.optimization_barrier(jnp.sum(edge_tensor * env_tensor, axis=0)) / root_five], axis=1).astype(jnp.bfloat16)
    update = jax.nn.silu(jnp.dot(invariants, scalar_proj, preferred_element_type=jnp.float32))
    latent_out = jnp.where(live[:, None], latent.astype(jnp.float32) + update, 0.0).astype(jnp.bfloat16)
    cross = jnp.stack([edge_vector[1] * env_vector[2] - edge_vector[2] * env_vector[1], edge_vector[2] * env_vector[0] - edge_vector[0] * env_vector[2], edge_vector[0] * env_vector[1] - edge_vector[1] * env_vector[0]])
    vector_out = path_gain[0][None, None, :] * scalar_part[None] * env_vector + path_gain[1][None, None, :] * edge_vector * env_scalar[None] + path_gain[2][None, None, :] * cross / root_two
    vector_out = jnp.where(live[None, :, None], vector_out, 0.0).astype(jnp.bfloat16)
    energy = lax.optimization_barrier(jnp.sum(latent_out.astype(jnp.float32) * energy_proj[None, :], axis=1))
    energy = jnp.where(live, energy, 0.0)
    return (latent_out, vector_out, energy)

def reference(atom_feat, atom_env, export_index, pair_vec, pair_center, pair_owner, pair_neigh, pair_count, center_proj, neighbour_proj, radial_proj, hidden_proj, split_proj, scalar_proj, path_gain, energy_proj):
    devices = N_GX * N_GY * N_GZ
    owners = N_GY * N_GZ
    owner_all = pair_owner[:, 0]

    def one_device(index):
        offset = index * PAIRS_DEV
        geometry = lax.dynamic_slice_in_dim(pair_vec, offset, PAIRS_DEV, 1)
        center = lax.dynamic_slice_in_dim(pair_center, offset, PAIRS_DEV, 0)
        owner = lax.dynamic_slice_in_dim(owner_all, offset, PAIRS_DEV, 0)
        neighbour = lax.dynamic_slice_in_dim(pair_neigh, offset, PAIRS_DEV, 0)
        owner_dev = index // owners * owners + owner
        center_row = owner_dev * ATOMS_DEV + center
        halo_slot = jnp.maximum(neighbour - ATOMS_DEV, 0)
        cell = halo_slot // EXPORT
        member = halo_slot % EXPORT
        source_x = (owner_dev // owners + cell // 9 - 1) % N_GX
        source_y = (owner_dev // N_GZ % N_GY + cell // 3 % 3 - 1) % N_GY
        source_z = (owner_dev % N_GZ + cell % 3 - 1) % N_GZ
        source = (source_x * N_GY + source_y) * N_GZ + source_z
        halo_row = source * ATOMS_DEV + export_index[source * EXPORT + member]
        neighbour_row = jnp.where(neighbour < ATOMS_DEV, owner_dev * ATOMS_DEV + neighbour, halo_row)
        live = jnp.arange(PAIRS_DEV, dtype=jnp.int32) < pair_count[index]
        latent_out, vector_out, energy = pair_block(atom_feat[center_row], atom_env[center_row], atom_feat[neighbour_row], geometry, live, center_proj, neighbour_proj, radial_proj, hidden_proj, split_proj, scalar_proj, path_gain, energy_proj)
        return (latent_out, vector_out, energy, center_row)
    latent_all, vector_all, energy_all, rows_all = lax.map(one_device, jnp.arange(devices, dtype=jnp.int32))
    pair_latent = latent_all.reshape(devices * PAIRS_DEV, latent_all.shape[-1])
    pair_vector = jnp.moveaxis(vector_all, 1, 0).reshape(3, devices * PAIRS_DEV, vector_all.shape[-1])
    atom_energy = jax.ops.segment_sum(energy_all.reshape(-1), rows_all.reshape(-1), num_segments=devices * ATOMS_DEV)
    return (pair_latent, pair_vector, atom_energy)
```

```python
import functools

import jax
import jax.numpy as jnp
from jax import lax
from jax.experimental import pallas as pl
from jax.experimental.pallas import tpu as pltpu
from jax.sharding import PartitionSpec as P

MESH = pl.DeviceIdType.MESH
F32 = jnp.float32
BF16 = jnp.bfloat16
GX, GY, GZ = 8, 4, 8
OWN = GY * GZ
CAP = 96
PAIRS = 2048
ATOMS = 1024
EXPORT = 256
CH = 128
LAT = 512
WIDTH = LAT + 3 * CH
ROWS = GY * CAP
SPACING = 6.0 / 7.0
R2, R3, R5, R15 = 2.0**0.5, 3.0**0.5, 5.0**0.5, 15.0**0.5

PEERS = [(dy, dz) for dz in range(GZ) for dy in range(GY) if (dy, dz) != (0, 0)]
CELLS = [(s // 9 - 1, s // 3 % 3 - 1, s % 3 - 1) for s in range(27)]
NEAR = [s for s in range(27) if s != 13]


def iota(shape, dim):
    return lax.broadcasted_iota(jnp.int32, shape, dim)


def parts(v):
    hi = v.astype(BF16)
    rest = v - hi.astype(F32)
    mid = rest.astype(BF16)
    lo = (rest - mid.astype(F32)).astype(BF16)
    return hi, mid, lo


def dot(a, b):
    return jnp.dot(a, b, preferred_element_type=F32)


def dot_t(a, b):
    return lax.dot_general(a, b, (((1,), (1,)), ((), ())), preferred_element_type=F32)


def wrapped(v, n):
    return lax.rem(v + n, n)


def request_kernel(
    count_ref,
    owner_ref,
    center_ref,
    neigh_ref,
    vec_ref,
    export_ref,
    feat_ref,
    req_ref,
    halo_ref,
    slot_ref,
    cidx_ref,
    nidx_ref,
    out_scr,
    exp_scr,
    req_send,
    req_recv,
    halo_send,
    halo_recv,
):
    x, y, z = lax.axis_index("gx"), lax.axis_index("gy"), lax.axis_index("gz")
    me = y * GZ + z
    barrier = pltpu.get_barrier_semaphore()
    for dy, dz in PEERS:
        pl.semaphore_signal(
            barrier,
            inc=1,
            device_id=(x, wrapped(y + dy, GY), wrapped(z + dz, GZ)),
            device_id_type=MESH,
        )
    for s in NEAR:
        ox, oy, oz = CELLS[s]
        pl.semaphore_signal(
            barrier,
            inc=1,
            device_id=(wrapped(x - ox, GX), wrapped(y - oy, GY), wrapped(z - oz, GZ)),
            device_id_type=MESH,
        )

    index8 = jnp.broadcast_to(export_ref[...].astype(F32), (8, EXPORT))
    index_col = jnp.transpose(index8)[:, :1]
    pick = jnp.where(index_col == iota((EXPORT, ATOMS), 1).astype(F32), 1.0, 0.0).astype(BF16)
    exp_scr[...] = dot(pick, feat_ref[...]).astype(BF16)

    owner = owner_ref[...]
    member = jnp.where(owner == iota((OWN, PAIRS), 0), 1.0, 0.0)
    member_b = member.astype(BF16)
    block = 256
    before = jnp.where(iota((block, block), 0) < iota((block, block), 1), 1.0, 0.0).astype(BF16)
    running = jnp.zeros((OWN, 1), F32)
    pieces = []
    for b in range(PAIRS // block):
        cut = member_b[:, b * block : (b + 1) * block]
        pieces.append(dot(cut, before) + running)
        running = running + jnp.sum(
            member[:, b * block : (b + 1) * block], axis=1, keepdims=True
        )
    earlier = jnp.concatenate(pieces, axis=1)
    rank = jnp.sum(member * earlier, axis=0, keepdims=True)
    slot_ref[...] = jnp.broadcast_to(owner.astype(F32) * CAP + rank, (8, PAIRS))

    live = iota((1, PAIRS), 1) < count_ref[0]
    code = jnp.where(live, center_ref[...] + 1, 0).astype(F32)
    near = neigh_ref[...].astype(F32)
    field = iota((8, PAIRS), 0)
    values = jnp.where(field == 0, code, jnp.where(field == 1, near, 0.0))
    for m in range(3):
        values = jnp.where(field == 2 + m, vec_ref[m : m + 1, :], values)
    at_rank = jnp.where(rank == iota((CH, PAIRS), 0).astype(F32), 1.0, 0.0).astype(BF16)
    packed = jnp.zeros((OWN * 8, CH), F32)
    for part in parts(values):
        wide = part.astype(F32)
        stacked = jnp.concatenate(
            [jnp.where(owner == o, wide, 0.0) for o in range(OWN)], axis=0
        ).astype(BF16)
        packed = packed + dot_t(stacked, at_rank)
    code_row = jnp.where(iota((8, CH), 0) == 0, 1.0, 0.0)
    for o in range(OWN):
        out_scr[o] = packed[o * 8 : (o + 1) * 8] - code_row

    pl.semaphore_wait(barrier, len(PEERS) + len(NEAR))
    copies = []
    for k, (dy, dz) in enumerate(PEERS):
        ty, tz = wrapped(y + dy, GY), wrapped(z + dz, GZ)
        copies.append(
            pltpu.make_async_remote_copy(
                src_ref=out_scr.at[ty * GZ + tz],
                dst_ref=req_ref.at[me],
                send_sem=req_send.at[k],
                recv_sem=req_recv.at[k],
                device_id=(x, ty, tz),
                device_id_type=MESH,
            )
        )
    for k, s in enumerate(NEAR):
        ox, oy, oz = CELLS[s]
        copies.append(
            pltpu.make_async_remote_copy(
                src_ref=exp_scr,
                dst_ref=halo_ref.at[s],
                send_sem=halo_send.at[k],
                recv_sem=halo_recv.at[k],
                device_id=(wrapped(x - ox, GX), wrapped(y - oy, GY), wrapped(z - oz, GZ)),
                device_id_type=MESH,
            )
        )
    for c in copies:
        c.start()
    halo_ref[13] = exp_scr[...]
    req_ref[me] = out_scr[me]
    for c in copies:
        c.wait()
    got = req_ref[...]
    cidx_ref[...] = jnp.maximum(got[:, 0, :], 0.0).astype(jnp.int32)
    nidx_ref[...] = got[:, 1, :].astype(jnp.int32)


def silu(v):
    return v * jax.nn.sigmoid(v)


def owner_kernel(
    cidx_ref,
    nidx_ref,
    req_ref,
    feat_ref,
    halo_ref,
    env_ref,
    center_proj,
    neighbour_proj,
    radial_proj,
    hidden_proj,
    split_proj,
    scalar_proj,
    gain_ref,
    energy_proj,
    back_ref,
    energy_ref,
    table,
    hc_scr,
    hn_scr,
    env_scr,
    cols,
    geo,
    send,
    send_sem,
    recv_sem,
    self_sem,
):
    x, y, z = lax.axis_index("gx"), lax.axis_index("gy"), lax.axis_index("gz")
    me = y * GZ + z
    barrier = pltpu.get_barrier_semaphore()
    for dy, dz in PEERS:
        pl.semaphore_signal(
            barrier,
            inc=1,
            device_id=(x, wrapped(y + dy, GY), wrapped(z + dz, GZ)),
            device_id_type=MESH,
        )
    table[0:ATOMS, :] = feat_ref[...].astype(F32)
    for s in range(27):
        table[ATOMS + s * EXPORT : ATOMS + (s + 1) * EXPORT, :] = halo_ref[s].astype(F32)
    energy_ref[...] = jnp.zeros_like(energy_ref)
    gain = gain_ref[...]
    weight = jnp.broadcast_to(energy_proj[...], (8, LAT))
    w_hi, w_mid, w_lo = parts(weight)
    row8 = iota((8, LAT), 0)
    w_parts = jnp.where(
        row8 == 0,
        w_hi.astype(F32),
        jnp.where(row8 == 1, w_mid.astype(F32), jnp.where(row8 == 2, w_lo.astype(F32), 0.0)),
    ).astype(BF16)

    def target(step, dy):
        h = lax.rem(step + 1, GZ)
        half = (h + 1) // 2
        dz = jnp.where(lax.rem(h, 2) == 1, GZ - half, half)
        return wrapped(y + dy, GY), wrapped(z + dz, GZ)

    def copy_of(step, dy):
        ty, tz = target(step, dy)
        k = step * GY + dy
        return pltpu.make_async_remote_copy(
            src_ref=send.at[k],
            dst_ref=back_ref.at[me],
            send_sem=send_sem.at[k],
            recv_sem=recv_sem.at[k],
            device_id=(x, ty, tz),
            device_id_type=MESH,
        )

    def self_copy(step):
        return pltpu.make_async_copy(send.at[step * GY], back_ref.at[me], self_sem)

    def group(step, carry):
        for dy in range(GY):
            ty, tz = target(step, dy)
            s = ty * GZ + tz
            rows = req_ref[s]
            vx, vy, vz = rows[2:3], rows[3:4], rows[4:5]
            length = jnp.sqrt(vx * vx + vy * vy + vz * vz)
            scale = jnp.maximum(length, 1.0)
            ux, uy, uz = vx / scale, vy / scale, vz / scale
            geo[0:1, :] = rows[0:1]
            geo[1:2, :] = R3 * ux
            geo[2:3, :] = R3 * uy
            geo[3:4, :] = R3 * uz
            geo[4:5, :] = R15 * ux * uy
            geo[5:6, :] = R15 * uy * uz
            geo[6:7, :] = 0.5 * R5 * (2.0 * uz * uz - ux * ux - uy * uy)
            geo[7:8, :] = R15 * ux * uz
            geo[8:9, :] = 0.5 * R15 * (ux * ux - uy * uy)
            centres = iota((8, CH), 0).astype(F32) * SPACING
            ratio = (length - centres) / SPACING
            geo[16:24, :] = jnp.exp(-(ratio * ratio))
            cols[dy * CAP : (dy + 1) * CAP, 0:32] = jnp.transpose(geo[...])[0:CAP, :]

            def fetch(i, c):
                for u in range(8):
                    r = i * 8 + u
                    at = dy * CAP + r
                    ci = cidx_ref[s, r]
                    hc_scr[pl.ds(at, 1), :] = table[pl.ds(ci, 1), :]
                    hn_scr[pl.ds(at, 1), :] = table[pl.ds(nidx_ref[s, r], 1), :]
                    env_scr[pl.ds(at * 16, 9), :] = env_ref[ci].astype(F32)
                return c

            lax.fori_loop(0, CAP // 8, fetch, 0)

        def col(k):
            return cols[:, k : k + 1]

        def env(m):
            return env_scr[pl.ds(m, ROWS, stride=16), :]

        code = col(0)
        live = code >= 0.0
        radial = cols[:, 16:24]
        radial_hi = radial.astype(BF16)
        radial_lo = (radial - radial_hi.astype(F32)).astype(BF16)
        pre = dot(hc_scr[...].astype(BF16), center_proj[...])
        pre = pre + dot(hn_scr[...].astype(BF16), neighbour_proj[...])
        pre = pre + dot(radial_hi, radial_proj[...]) + dot(radial_lo, radial_proj[...])
        hidden = silu(pre).astype(BF16)
        latent = silu(dot(hidden, hidden_proj[...])).astype(BF16)
        mixed = dot(latent, split_proj[...])
        z0, z1, z2 = mixed[:, :CH], mixed[:, CH : 2 * CH], mixed[:, 2 * CH :]
        e0, ex, ey, ez = env(0), env(1), env(2), env(3)
        yx, yy, yz = col(1), col(2), col(3)
        first = (yx * ex + yy * ey + yz * ez) * (1.0 / R3)
        second = col(4) * env(4)
        for m in range(1, 5):
            second = second + col(4 + m) * env(4 + m)
        second = second * (1.0 / R5)
        invariants = jnp.concatenate([z0 * e0, z1 * first, z2 * second], axis=1).astype(BF16)
        update = silu(dot(invariants, scalar_proj[...]))
        out = jnp.where(live, latent.astype(F32) + update, 0.0).astype(BF16)
        a = gain[0:1] * z0
        b = gain[1:2] * z1 * e0
        c = (gain[2:3] * (1.0 / R2)) * z1
        ux = a * ex + b * yx + c * (yy * ez - yz * ey)
        uy = a * ey + b * yy + c * (yz * ex - yx * ez)
        uz = a * ez + b * yz + c * (yx * ey - yy * ex)
        vectors = [jnp.where(live, v, 0.0).astype(BF16) for v in (ux, uy, uz)]
        for dy in range(GY):
            k = step * GY + dy
            cut = slice(dy * CAP, (dy + 1) * CAP)
            send[k, :, 0:LAT] = out[cut]
            for m in range(3):
                send[k, :, LAT + m * CH : LAT + (m + 1) * CH] = vectors[m][cut]

        @pl.when(step == 0)
        def _():
            pl.semaphore_wait(barrier, len(PEERS))

        for dy in range(1, GY):
            copy_of(step, dy).start()

        @pl.when(step < GZ - 1)
        def _():
            copy_of(step, 0).start()

        @pl.when(step == GZ - 1)
        def _():
            self_copy(step).start()

        pair_energy = jnp.sum(dot_t(w_parts, out), axis=0, keepdims=True)
        e_hi, e_mid, e_lo = parts(jnp.broadcast_to(pair_energy, (8, ROWS)))
        row = iota((8, ROWS), 0)
        e_parts = jnp.where(
            row == 0,
            e_hi.astype(F32),
            jnp.where(row == 1, e_mid.astype(F32), jnp.where(row == 2, e_lo.astype(F32), 0.0)),
        ).astype(BF16)
        onehot = jnp.where(code == iota((ROWS, ATOMS), 1).astype(F32), 1.0, 0.0).astype(BF16)
        energy_ref[...] += dot(e_parts, onehot)
        return carry

    lax.fori_loop(0, GZ, group, 0)

    def finish(step, carry):
        for dy in range(1, GY):
            copy_of(step, dy).wait()

        @pl.when(step < GZ - 1)
        def _():
            copy_of(step, 0).wait()

        @pl.when(step == GZ - 1)
        def _():
            self_copy(step).wait()

        return carry

    lax.fori_loop(0, GZ, finish, 0)


def return_kernel(slot_ref, back_ref, latent_ref, vector_ref):
    col = jnp.transpose(slot_ref[...])[:, :1]
    pick = jnp.where(col == iota((256, OWN * CAP), 1).astype(F32), 1.0, 0.0).astype(BF16)
    got = dot(pick, back_ref[...]).astype(BF16)
    latent_ref[...] = got[:, :LAT]
    for m in range(3):
        vector_ref[m] = got[:, LAT + m * CH : LAT + (m + 1) * CH]


def vmem():
    return pl.BlockSpec(memory_space=pltpu.VMEM)


def smem():
    return pl.BlockSpec(memory_space=pltpu.SMEM)


def shaped(shape, dtype):
    return jax.ShapeDtypeStruct(shape, dtype)


def local(
    atom_feat,
    atom_env,
    export_index,
    pair_vec,
    pair_center,
    pair_owner,
    pair_neigh,
    pair_count,
    center_proj,
    neighbour_proj,
    radial_proj,
    hidden_proj,
    split_proj,
    scalar_proj,
    path_gain,
    energy_proj,
):
    req, halo, slot, cidx, nidx = pl.pallas_call(
        request_kernel,
        out_shape=(
            shaped((OWN, 8, CH), F32),
            shaped((27, EXPORT, CH), BF16),
            shaped((8, PAIRS), F32),
            shaped((OWN, CH), jnp.int32),
            shaped((OWN, CH), jnp.int32),
        ),
        in_specs=[smem()] + [vmem()] * 6,
        out_specs=tuple([vmem()] * 5),
        scratch_shapes=[
            pltpu.VMEM((OWN, 8, CH), F32),
            pltpu.VMEM((EXPORT, CH), BF16),
            pltpu.SemaphoreType.DMA((31,)),
            pltpu.SemaphoreType.DMA((31,)),
            pltpu.SemaphoreType.DMA((26,)),
            pltpu.SemaphoreType.DMA((26,)),
        ],
        compiler_params=pltpu.CompilerParams(collective_id=0, has_side_effects=True),
    )(
        pair_count,
        pair_owner.reshape(1, PAIRS),
        pair_center.reshape(1, PAIRS),
        pair_neigh.reshape(1, PAIRS),
        pair_vec,
        export_index.reshape(1, EXPORT),
        atom_feat,
    )
    back, energy = pl.pallas_call(
        owner_kernel,
        out_shape=(shaped((OWN, CAP, WIDTH), BF16), shaped((8, ATOMS), F32)),
        in_specs=[smem()] * 2 + [vmem()] * 12,
        out_specs=(pl.BlockSpec(memory_space=pl.ANY), vmem()),
        scratch_shapes=[
            pltpu.VMEM((ATOMS + 27 * EXPORT, CH), F32),
            pltpu.VMEM((ROWS, CH), F32),
            pltpu.VMEM((ROWS, CH), F32),
            pltpu.VMEM((ROWS * 16, CH), F32),
            pltpu.VMEM((ROWS, CH), F32),
            pltpu.VMEM((32, CH), F32),
            pltpu.VMEM((OWN, CAP, WIDTH), BF16),
            pltpu.SemaphoreType.DMA((OWN,)),
            pltpu.SemaphoreType.DMA((OWN,)),
            pltpu.SemaphoreType.DMA,
        ],
        compiler_params=pltpu.CompilerParams(
            collective_id=1, has_side_effects=True, vmem_limit_bytes=56 * 1024 * 1024
        ),
    )(
        cidx,
        nidx,
        req,
        atom_feat,
        halo,
        atom_env,
        center_proj,
        neighbour_proj,
        radial_proj,
        hidden_proj,
        split_proj,
        scalar_proj,
        path_gain,
        energy_proj.reshape(1, LAT),
    )
    latent, vector = pl.pallas_call(
        return_kernel,
        grid=(PAIRS // 256,),
        out_shape=(shaped((PAIRS, LAT), BF16), shaped((3, PAIRS, CH), BF16)),
        in_specs=[
            pl.BlockSpec((8, 256), lambda i: (0, i)),
            pl.BlockSpec((OWN * CAP, WIDTH), lambda i: (0, 0)),
        ],
        out_specs=(
            pl.BlockSpec((256, LAT), lambda i: (i, 0)),
            pl.BlockSpec((3, 256, CH), lambda i: (0, i, 0)),
        ),
        compiler_params=pltpu.CompilerParams(vmem_limit_bytes=40 * 1024 * 1024),
    )(slot, back.reshape(OWN * CAP, WIDTH))
    return (latent, vector, jnp.sum(energy, axis=0))


def solution(mesh):
    rows = ("gx", "gy", "gz")
    placed = (
        P(rows, None),
        P(rows, None, None),
        P(rows),
        P(None, rows),
        P(rows),
        P(rows, None),
        P(rows),
        P(rows),
    ) + (P(),) * 8
    return jax.shard_map(
        local,
        mesh=mesh,
        in_specs=placed,
        out_specs=(P(rows, None), P(None, rows, None), P(rows)),
        check_vma=False,
    )
```

```python
import functools

import jax
import jax.numpy as jnp
from jax import lax
from jax.experimental import pallas as pl
from jax.experimental.pallas import tpu as pltpu
from jax.sharding import PartitionSpec as P

MESH = pl.DeviceIdType.MESH
F32 = jnp.float32
BF16 = jnp.bfloat16
GX, GY, GZ = 8, 4, 8
OWN = GY * GZ
CAP = 96
PAIRS = 2048
ATOMS = 1024
EXPORT = 256
CH = 128
LAT = 512
WIDTH = LAT + 3 * CH
ROWS = GY * CAP
SPACING = 6.0 / 7.0
R2, R3, R5, R15 = 2.0**0.5, 3.0**0.5, 5.0**0.5, 15.0**0.5

PEERS = [(dy, dz) for dz in range(GZ) for dy in range(GY) if (dy, dz) != (0, 0)]
AROUND = [(oy, oz) for oy in (-1, 0, 1) for oz in (-1, 0, 1) if (oy, oz) != (0, 0)]


def iota(shape, dim):
    return lax.broadcasted_iota(jnp.int32, shape, dim)


def parts(v):
    hi = v.astype(BF16)
    rest = v - hi.astype(F32)
    mid = rest.astype(BF16)
    lo = (rest - mid.astype(F32)).astype(BF16)
    return hi, mid, lo


def dot(a, b):
    return jnp.dot(a, b, preferred_element_type=F32)


def dot_t(a, b):
    return lax.dot_general(a, b, (((1,), (1,)), ((), ())), preferred_element_type=F32)


def wrapped(v, n):
    return lax.rem(v + n, n)


def request_kernel(
    count_ref,
    owner_ref,
    center_ref,
    neigh_ref,
    vec_ref,
    export_ref,
    feat_ref,
    req_ref,
    halo_ref,
    slot_ref,
    nidx_ref,
    out_scr,
    req_send,
    req_recv,
    halo_send,
    halo_recv,
):
    x, y, z = lax.axis_index("gx"), lax.axis_index("gy"), lax.axis_index("gz")
    me = y * GZ + z
    barrier = pltpu.get_barrier_semaphore()
    for dy, dz in PEERS:
        pl.semaphore_signal(
            barrier,
            inc=1,
            device_id=(x, wrapped(y + dy, GY), wrapped(z + dz, GZ)),
            device_id_type=MESH,
        )
    for side in (1, -1):
        pl.semaphore_signal(
            barrier,
            inc=1,
            device_id=(wrapped(x + side, GX), y, z),
            device_id_type=MESH,
        )

    index8 = jnp.broadcast_to(export_ref[...].astype(F32), (8, EXPORT))
    index_col = jnp.transpose(index8)[:, :1]
    pick = jnp.where(index_col == iota((EXPORT, ATOMS), 1).astype(F32), 1.0, 0.0).astype(BF16)
    halo_ref[13] = dot(pick, feat_ref[...]).astype(BF16)

    owner = owner_ref[...]
    member = jnp.where(owner == iota((OWN, PAIRS), 0), 1.0, 0.0)
    member_b = member.astype(BF16)
    block = 256
    before = jnp.where(iota((block, block), 0) < iota((block, block), 1), 1.0, 0.0).astype(BF16)
    running = jnp.zeros((OWN, 1), F32)
    pieces = []
    for b in range(PAIRS // block):
        cut = member_b[:, b * block : (b + 1) * block]
        pieces.append(dot(cut, before) + running)
        running = running + jnp.sum(
            member[:, b * block : (b + 1) * block], axis=1, keepdims=True
        )
    earlier = jnp.concatenate(pieces, axis=1)
    rank = jnp.sum(member * earlier, axis=0, keepdims=True)
    slot_ref[...] = jnp.broadcast_to(owner.astype(F32) * CAP + rank, (8, PAIRS))

    live = iota((1, PAIRS), 1) < count_ref[0]
    code = jnp.where(live, center_ref[...] + 1, 0).astype(F32)
    near = neigh_ref[...].astype(F32)
    field = iota((8, PAIRS), 0)
    values = jnp.where(field == 0, code, jnp.where(field == 1, near, 0.0))
    for m in range(3):
        values = jnp.where(field == 2 + m, vec_ref[m : m + 1, :], values)
    at_rank = jnp.where(rank == iota((CH, PAIRS), 0).astype(F32), 1.0, 0.0).astype(BF16)
    packed = jnp.zeros((OWN * 8, CH), F32)
    for part in parts(values):
        wide = part.astype(F32)
        stacked = jnp.concatenate(
            [jnp.where(owner == o, wide, 0.0) for o in range(OWN)], axis=0
        ).astype(BF16)
        packed = packed + dot_t(stacked, at_rank)
    code_row = jnp.where(iota((8, CH), 0) == 0, 1.0, 0.0)
    for o in range(OWN):
        out_scr[o] = packed[o * 8 : (o + 1) * 8] - code_row

    pl.semaphore_wait(barrier, len(PEERS) + 2)
    plane, requests, sides = [], [], []
    for k, (oy, oz) in enumerate(AROUND):
        plane.append(
            pltpu.make_async_remote_copy(
                src_ref=halo_ref.at[13],
                dst_ref=halo_ref.at[13 + 3 * oy + oz],
                send_sem=halo_send.at[k],
                recv_sem=halo_recv.at[k],
                device_id=(x, wrapped(y - oy, GY), wrapped(z - oz, GZ)),
                device_id_type=MESH,
            )
        )
    for k, (dy, dz) in enumerate(PEERS):
        ty, tz = wrapped(y + dy, GY), wrapped(z + dz, GZ)
        requests.append(
            pltpu.make_async_remote_copy(
                src_ref=out_scr.at[ty * GZ + tz],
                dst_ref=req_ref.at[me],
                send_sem=req_send.at[k],
                recv_sem=req_recv.at[k],
                device_id=(x, ty, tz),
                device_id_type=MESH,
            )
        )
    for k, side in enumerate((1, -1)):
        sides.append(
            pltpu.make_async_remote_copy(
                src_ref=halo_ref.at[9:18],
                dst_ref=halo_ref.at[0:9] if side == 1 else halo_ref.at[18:27],
                send_sem=halo_send.at[8 + k],
                recv_sem=halo_recv.at[8 + k],
                device_id=(wrapped(x + side, GX), y, z),
                device_id_type=MESH,
            )
        )
    for c in plane + requests:
        c.start()
    req_ref[me] = out_scr[me]
    for c in plane:
        c.wait()
    for c in sides:
        c.start()
    for c in requests:
        c.wait()
    got = req_ref[...]
    nidx_ref[...] = got[:, 1, :].astype(jnp.int32)
    for c in sides:
        c.wait()


def silu(v):
    return v * jax.nn.sigmoid(v)


def owner_kernel(
    nidx_ref,
    req_ref,
    slot_ref,
    feat_ref,
    halo_ref,
    env_ref,
    center_proj,
    neighbour_proj,
    radial_proj,
    hidden_proj,
    split_proj,
    scalar_proj,
    gain_ref,
    energy_proj,
    latent_ref,
    vector_ref,
    energy_ref,
    table,
    hn_scr,
    center,
    slot_col,
    cols,
    geo,
    send,
    recv,
    send_sem,
    recv_sem,
):
    x, y, z = lax.axis_index("gx"), lax.axis_index("gy"), lax.axis_index("gz")
    me = y * GZ + z
    barrier = pltpu.get_barrier_semaphore()
    for dy, dz in PEERS:
        pl.semaphore_signal(
            barrier,
            inc=1,
            device_id=(x, wrapped(y + dy, GY), wrapped(z + dz, GZ)),
            device_id_type=MESH,
        )
    table[0:ATOMS, :] = feat_ref[...].astype(F32)
    for s in range(27):
        table[ATOMS + s * EXPORT : ATOMS + (s + 1) * EXPORT, :] = halo_ref[s].astype(F32)
    for m in range(9):
        center[:, m * CH : (m + 1) * CH] = env_ref[m]
    center[:, 9 * CH :] = feat_ref[...]
    energy_ref[...] = jnp.zeros_like(energy_ref)
    gain = gain_ref[...]
    weight = jnp.broadcast_to(energy_proj[...], (8, LAT))
    w_hi, w_mid, w_lo = parts(weight)
    row8 = iota((8, LAT), 0)
    w_parts = jnp.where(
        row8 == 0,
        w_hi.astype(F32),
        jnp.where(row8 == 1, w_mid.astype(F32), jnp.where(row8 == 2, w_lo.astype(F32), 0.0)),
    ).astype(BF16)

    def target(step, dy):
        h = lax.rem(step + 1, GZ)
        half = (h + 1) // 2
        dz = jnp.where(lax.rem(h, 2) == 1, GZ - half, half)
        return wrapped(y + dy, GY), wrapped(z + dz, GZ)

    def copy_of(step, dy):
        ty, tz = target(step, dy)
        k = step * GY + dy
        return pltpu.make_async_remote_copy(
            src_ref=send.at[k],
            dst_ref=recv.at[k],
            send_sem=send_sem.at[k],
            recv_sem=recv_sem.at[k],
            device_id=(x, ty, tz),
            device_id_type=MESH,
        )

    def group(step, carry):
        for dy in range(GY):
            ty, tz = target(step, dy)
            s = ty * GZ + tz
            rows = req_ref[s]
            vx, vy, vz = rows[2:3], rows[3:4], rows[4:5]
            length = jnp.sqrt(vx * vx + vy * vy + vz * vz)
            scale = jnp.maximum(length, 1.0)
            ux, uy, uz = vx / scale, vy / scale, vz / scale
            geo[0:1, :] = rows[0:1]
            geo[1:2, :] = R3 * ux
            geo[2:3, :] = R3 * uy
            geo[3:4, :] = R3 * uz
            geo[4:5, :] = R15 * ux * uy
            geo[5:6, :] = R15 * uy * uz
            geo[6:7, :] = 0.5 * R5 * (2.0 * uz * uz - ux * ux - uy * uy)
            geo[7:8, :] = R15 * ux * uz
            geo[8:9, :] = 0.5 * R15 * (ux * ux - uy * uy)
            centres = iota((8, CH), 0).astype(F32) * SPACING
            ratio = (length - centres) / SPACING
            geo[16:24, :] = jnp.exp(-(ratio * ratio))
            cols[dy * CAP : (dy + 1) * CAP, 0:32] = jnp.transpose(geo[...])[0:CAP, :]

            def fetch(i, c):
                for u in range(16):
                    r = i * 16 + u
                    hn_scr[pl.ds(dy * CAP + r, 1), :] = table[pl.ds(nidx_ref[s, r], 1), :]
                return c

            lax.fori_loop(0, CAP // 16, fetch, 0)

        def col(k):
            return cols[:, k : k + 1]

        code = col(0)
        live = code >= 0.0
        onehot = jnp.where(code == iota((ROWS, ATOMS), 1).astype(F32), 1.0, 0.0).astype(BF16)
        fetched = dot(onehot, center[...])

        def env(m):
            return fetched[:, m * CH : (m + 1) * CH]

        radial = cols[:, 16:24]
        radial_hi = radial.astype(BF16)
        radial_lo = (radial - radial_hi.astype(F32)).astype(BF16)
        pre = dot(env(9).astype(BF16), center_proj[...])
        pre = pre + dot(hn_scr[...].astype(BF16), neighbour_proj[...])
        pre = pre + dot(radial_hi, radial_proj[...]) + dot(radial_lo, radial_proj[...])
        hidden = silu(pre).astype(BF16)
        latent = silu(dot(hidden, hidden_proj[...])).astype(BF16)
        mixed = dot(latent, split_proj[...])
        z0, z1, z2 = mixed[:, :CH], mixed[:, CH : 2 * CH], mixed[:, 2 * CH :]
        e0, ex, ey, ez = env(0), env(1), env(2), env(3)
        yx, yy, yz = col(1), col(2), col(3)
        first = (yx * ex + yy * ey + yz * ez) * (1.0 / R3)
        second = col(4) * env(4)
        for m in range(1, 5):
            second = second + col(4 + m) * env(4 + m)
        second = second * (1.0 / R5)
        invariants = jnp.concatenate([z0 * e0, z1 * first, z2 * second], axis=1).astype(BF16)
        update = silu(dot(invariants, scalar_proj[...]))
        out = jnp.where(live, latent.astype(F32) + update, 0.0).astype(BF16)
        a = gain[0:1] * z0
        b = gain[1:2] * z1 * e0
        c = (gain[2:3] * (1.0 / R2)) * z1
        ux = a * ex + b * yx + c * (yy * ez - yz * ey)
        uy = a * ey + b * yy + c * (yz * ex - yx * ez)
        uz = a * ez + b * yz + c * (yx * ey - yy * ex)
        vectors = [jnp.where(live, v, 0.0).astype(BF16) for v in (ux, uy, uz)]
        for dy in range(GY):
            k = step * GY + dy
            cut = slice(dy * CAP, (dy + 1) * CAP)
            send[k, :, 0:LAT] = out[cut]
            for m in range(3):
                send[k, :, LAT + m * CH : LAT + (m + 1) * CH] = vectors[m][cut]

        @pl.when(step == 0)
        def _():
            pl.semaphore_wait(barrier, len(PEERS))

        for dy in range(1, GY):
            copy_of(step, dy).start()

        @pl.when(step < GZ - 1)
        def _():
            copy_of(step, 0).start()

        @pl.when(step == GZ - 1)
        def _():
            recv[step * GY] = send[step * GY]

        pair_energy = jnp.sum(dot_t(w_parts, out), axis=0, keepdims=True)
        e_hi, e_mid, e_lo = parts(jnp.broadcast_to(pair_energy, (8, ROWS)))
        row = iota((8, ROWS), 0)
        e_parts = jnp.where(
            row == 0,
            e_hi.astype(F32),
            jnp.where(row == 1, e_mid.astype(F32), jnp.where(row == 2, e_lo.astype(F32), 0.0)),
        ).astype(BF16)
        energy_ref[...] += dot(e_parts, onehot)
        return carry

    lax.fori_loop(0, GZ, group, 0)

    slot_col[...] = jnp.transpose(slot_ref[...])
    latent_ref[...] = jnp.zeros_like(latent_ref)
    vector_ref[...] = jnp.zeros_like(vector_ref)

    def arrive(turn, carry):
        step = jnp.where(turn == 6, 7, jnp.where(turn == 7, 6, turn))
        for dy in range(1, GY):
            copy_of(step, dy).wait_recv()

        @pl.when(step < GZ - 1)
        def _():
            copy_of(step, 0).wait_recv()

        h = lax.rem(step + 1, GZ)
        half = (h + 1) // 2
        dz = jnp.where(lax.rem(h, 2) == 1, GZ - half, half)
        sz = wrapped(z - dz, GZ)
        lane = iota((8, ROWS), 1)
        wanted = lane
        for dy in range(GY):
            base = (wrapped(y - dy, GY) * GZ + sz) * CAP - dy * CAP
            wanted = jnp.where((lane >= dy * CAP) & (lane < (dy + 1) * CAP), lane + base, wanted)
        wanted = wanted[0:1].astype(F32)
        rows = recv[pl.ds(step * GY, GY)].reshape(ROWS, WIDTH)

        def block(i, c):
            at = pl.ds(pl.multiple_of(i * 256, 256), 256)
            col = slot_col[at, 0:1]
            got = dot(jnp.where(col == wanted, 1.0, 0.0).astype(BF16), rows)
            latent_ref[at, :] = (latent_ref[at, :].astype(F32) + got[:, :LAT]).astype(BF16)
            for m in range(3):
                part = got[:, LAT + m * CH : LAT + (m + 1) * CH]
                vector_ref[m, at, :] = (vector_ref[m, at, :].astype(F32) + part).astype(BF16)
            return c

        lax.fori_loop(0, PAIRS // 256, block, 0)
        return carry

    lax.fori_loop(0, GZ, arrive, 0)

    def finish(step, carry):
        for dy in range(1, GY):
            copy_of(step, dy).wait_send()

        @pl.when(step < GZ - 1)
        def _():
            copy_of(step, 0).wait_send()

        return carry

    lax.fori_loop(0, GZ, finish, 0)


def vmem():
    return pl.BlockSpec(memory_space=pltpu.VMEM)


def smem():
    return pl.BlockSpec(memory_space=pltpu.SMEM)


def shaped(shape, dtype):
    return jax.ShapeDtypeStruct(shape, dtype)


def local(
    atom_feat,
    atom_env,
    export_index,
    pair_vec,
    pair_center,
    pair_owner,
    pair_neigh,
    pair_count,
    center_proj,
    neighbour_proj,
    radial_proj,
    hidden_proj,
    split_proj,
    scalar_proj,
    path_gain,
    energy_proj,
):
    req, halo, slot, nidx = pl.pallas_call(
        request_kernel,
        out_shape=(
            shaped((OWN, 8, CH), F32),
            shaped((27, EXPORT, CH), BF16),
            shaped((8, PAIRS), F32),
            shaped((OWN, CH), jnp.int32),
        ),
        in_specs=[smem()] + [vmem()] * 6,
        out_specs=tuple([vmem()] * 4),
        scratch_shapes=[
            pltpu.VMEM((OWN, 8, CH), F32),
            pltpu.SemaphoreType.DMA((31,)),
            pltpu.SemaphoreType.DMA((31,)),
            pltpu.SemaphoreType.DMA((10,)),
            pltpu.SemaphoreType.DMA((10,)),
        ],
        compiler_params=pltpu.CompilerParams(collective_id=0, has_side_effects=True),
    )(
        pair_count,
        pair_owner.reshape(1, PAIRS),
        pair_center.reshape(1, PAIRS),
        pair_neigh.reshape(1, PAIRS),
        pair_vec,
        export_index.reshape(1, EXPORT),
        atom_feat,
    )
    latent, vector, energy = pl.pallas_call(
        owner_kernel,
        out_shape=(
            shaped((PAIRS, LAT), BF16),
            shaped((3, PAIRS, CH), BF16),
            shaped((8, ATOMS), F32),
        ),
        in_specs=[smem()] + [vmem()] * 13,
        out_specs=tuple([vmem()] * 3),
        scratch_shapes=[
            pltpu.VMEM((ATOMS + 27 * EXPORT, CH), F32),
            pltpu.VMEM((ROWS, CH), F32),
            pltpu.VMEM((ATOMS, 10 * CH), BF16),
            pltpu.VMEM((PAIRS, 8), F32),
            pltpu.VMEM((ROWS, CH), F32),
            pltpu.VMEM((32, CH), F32),
            pltpu.VMEM((OWN, CAP, WIDTH), BF16),
            pltpu.VMEM((OWN, CAP, WIDTH), BF16),
            pltpu.SemaphoreType.DMA((OWN,)),
            pltpu.SemaphoreType.DMA((OWN,)),
        ],
        compiler_params=pltpu.CompilerParams(
            collective_id=1, has_side_effects=True, vmem_limit_bytes=60000 * 1024
        ),
    )(
        nidx,
        req,
        slot,
        atom_feat,
        halo,
        jnp.moveaxis(atom_env, 1, 0),
        center_proj,
        neighbour_proj,
        radial_proj,
        hidden_proj,
        split_proj,
        scalar_proj,
        path_gain,
        energy_proj.reshape(1, LAT),
    )
    return (latent, vector, jnp.sum(energy, axis=0))


def solution(mesh):
    rows = ("gx", "gy", "gz")
    placed = (
        P(rows, None),
        P(rows, None, None),
        P(rows),
        P(None, rows),
        P(rows),
        P(rows, None),
        P(rows),
        P(rows),
    ) + (P(),) * 8
    return jax.shard_map(
        local,
        mesh=mesh,
        in_specs=placed,
        out_specs=(P(rows, None), P(None, rows, None), P(rows)),
        check_vma=False,
    )
```

```python
import jax
import jax.numpy as jnp
from jax import lax
from jax.experimental import pallas as pl
from jax.experimental.pallas import tpu as pltpu
from jax.sharding import PartitionSpec as P

MESH = pl.DeviceIdType.MESH
F32 = jnp.float32
BF16 = jnp.bfloat16
GX, GY, GZ = 8, 4, 8
OWN = GY * GZ
CAP = 96
PAIRS = 2048
ATOMS = 1024
EXPORT = 256
CH = 128
LAT = 512
WIDTH = LAT + 3 * CH
ROWS = GY * CAP
SPACING = 6.0 / 7.0
R2, R3, R5, R15 = 2.0**0.5, 3.0**0.5, 5.0**0.5, 15.0**0.5

PEERS = [(dy, dz) for dz in range(GZ) for dy in range(GY) if (dy, dz) != (0, 0)]
AROUND = [(oy, oz) for oy in (-1, 0, 1) for oz in (-1, 0, 1) if (oy, oz) != (0, 0)]


def iota(shape, dim):
    return lax.broadcasted_iota(jnp.int32, shape, dim)


def parts(v):
    hi = v.astype(BF16)
    rest = v - hi.astype(F32)
    mid = rest.astype(BF16)
    lo = (rest - mid.astype(F32)).astype(BF16)
    return hi, mid, lo


def dot(a, b):
    return jnp.dot(a, b, preferred_element_type=F32)


def dot_t(a, b):
    return lax.dot_general(a, b, (((1,), (1,)), ((), ())), preferred_element_type=F32)


def wrapped(v, n):
    return lax.rem(v + n, n)


def silu(v):
    return v * jax.nn.sigmoid(v)


def layer_kernel(
    count_ref,
    owner_ref,
    center_ref,
    neigh_ref,
    vec_ref,
    export_ref,
    feat_ref,
    env_ref,
    center_proj,
    neighbour_proj,
    radial_proj,
    hidden_proj,
    split_proj,
    scalar_proj,
    gain_ref,
    energy_proj,
    acc_ref,
    last_ref,
    wanted_ref,
    slot_ref,
    energy_ref,
    ask,
    req,
    halo,
    center,
    slot_col,
    cols,
    geo,
    send,
    recv,
    load_sem,
    req_send,
    req_recv,
    halo_send,
    halo_recv,
    side_send,
    side_recv,
    send_sem,
    recv_sem,
):
    x, y, z = lax.axis_index("gx"), lax.axis_index("gy"), lax.axis_index("gz")
    me = y * GZ + z
    barrier = pltpu.get_barrier_semaphore()
    for dy, dz in PEERS:
        pl.semaphore_signal(
            barrier,
            inc=1,
            device_id=(x, wrapped(y + dy, GY), wrapped(z + dz, GZ)),
            device_id_type=MESH,
        )
    for side in (1, -1):
        pl.semaphore_signal(
            barrier,
            inc=1,
            device_id=(wrapped(x + side, GX), y, z),
            device_id_type=MESH,
        )

    loads = [
        pltpu.make_async_copy(env_ref.at[m], center.at[:, m * CH : (m + 1) * CH], load_sem.at[m])
        for m in range(9)
    ]
    loads.append(pltpu.make_async_copy(feat_ref, center.at[:, 9 * CH :], load_sem.at[9]))
    for c in reversed(loads):
        c.start()

    index8 = jnp.broadcast_to(export_ref[...].astype(F32), (8, EXPORT))
    index_col = jnp.transpose(index8)[:, :1]
    pick = jnp.where(index_col == iota((EXPORT, ATOMS), 1).astype(F32), 1.0, 0.0).astype(BF16)
    loads[9].wait()
    halo[13] = dot(pick, center[:, 9 * CH :]).astype(BF16)

    owner = owner_ref[...]
    member = jnp.where(owner == iota((OWN, PAIRS), 0), 1.0, 0.0)
    member_b = member.astype(BF16)
    block = 256
    before = jnp.where(iota((block, block), 0) < iota((block, block), 1), 1.0, 0.0).astype(BF16)
    running = jnp.zeros((OWN, 1), F32)
    pieces = []
    for b in range(PAIRS // block):
        cut = member_b[:, b * block : (b + 1) * block]
        pieces.append(dot(cut, before) + running)
        running = running + jnp.sum(
            member[:, b * block : (b + 1) * block], axis=1, keepdims=True
        )
    earlier = jnp.concatenate(pieces, axis=1)
    rank = jnp.sum(member * earlier, axis=0, keepdims=True)
    slot_ref[...] = jnp.broadcast_to(owner.astype(F32) * CAP + rank, (8, PAIRS))

    live = iota((1, PAIRS), 1) < count_ref[0]
    code = jnp.where(live, center_ref[...] + 1, 0).astype(F32)
    near = neigh_ref[...].astype(F32)
    field = iota((8, PAIRS), 0)
    values = jnp.where(field == 0, code, jnp.where(field == 1, near, 0.0))
    for m in range(3):
        values = jnp.where(field == 2 + m, vec_ref[m : m + 1, :], values)
    at_rank = jnp.where(rank == iota((CH, PAIRS), 0).astype(F32), 1.0, 0.0).astype(BF16)
    packed = jnp.zeros((OWN * 8, CH), F32)
    for part in parts(values):
        wide = part.astype(F32)
        stacked = jnp.concatenate(
            [jnp.where(owner == o, wide, 0.0) for o in range(OWN)], axis=0
        ).astype(BF16)
        packed = packed + dot_t(stacked, at_rank)
    code_row = jnp.where(iota((8, CH), 0) == 0, 1.0, 0.0)
    for o in range(OWN):
        ask[o] = packed[o * 8 : (o + 1) * 8] - code_row

    pl.semaphore_wait(barrier, len(PEERS) + 2)
    plane, requests, sides = [], [], []
    for k, (oy, oz) in enumerate(AROUND):
        plane.append(
            pltpu.make_async_remote_copy(
                src_ref=halo.at[13],
                dst_ref=halo.at[13 + 3 * oy + oz],
                send_sem=halo_send.at[k],
                recv_sem=halo_recv.at[k],
                device_id=(x, wrapped(y - oy, GY), wrapped(z - oz, GZ)),
                device_id_type=MESH,
            )
        )
    for k, (dy, dz) in enumerate(PEERS):
        ty, tz = wrapped(y + dy, GY), wrapped(z + dz, GZ)
        requests.append(
            pltpu.make_async_remote_copy(
                src_ref=ask.at[ty * GZ + tz],
                dst_ref=req.at[me],
                send_sem=req_send.at[k],
                recv_sem=req_recv.at[k],
                device_id=(x, ty, tz),
                device_id_type=MESH,
            )
        )
    for k, (oy, oz) in enumerate(((0, 0),) + tuple(AROUND)):
        cell = 13 + 3 * oy + oz
        for e, side in enumerate((1, -1)):
            sides.append(
                pltpu.make_async_remote_copy(
                    src_ref=halo.at[cell],
                    dst_ref=halo.at[cell - 9 * side],
                    send_sem=side_send.at[2 * k + e],
                    recv_sem=side_recv.at[2 * k + e],
                    device_id=(wrapped(x + side, GX), y, z),
                    device_id_type=MESH,
                )
            )
    for c in plane + sides[:2] + requests:
        c.start()
    req[me] = ask[me]
    for k, c in enumerate(plane):
        c.wait_recv()
        sides[2 * k + 2].start()
        sides[2 * k + 3].start()
    for c in requests:
        c.wait_recv()
    for c in plane + requests:
        c.wait_send()
    for c in loads[:9]:
        c.wait()

    energy_ref[...] = jnp.zeros_like(energy_ref)
    gain = gain_ref[...]
    weight = jnp.broadcast_to(energy_proj[...], (8, LAT))
    w_hi, w_mid, w_lo = parts(weight)
    row8 = iota((8, LAT), 0)
    w_parts = jnp.where(
        row8 == 0,
        w_hi.astype(F32),
        jnp.where(row8 == 1, w_mid.astype(F32), jnp.where(row8 == 2, w_lo.astype(F32), 0.0)),
    ).astype(BF16)

    slot_col[...] = jnp.transpose(slot_ref[...])
    acc_ref[...] = jnp.zeros_like(acc_ref)
    for c in sides:
        c.wait()

    def target(step, dy):
        h = lax.rem(step + 1, GZ)
        half = (h + 1) // 2
        dz = jnp.where(lax.rem(h, 2) == 1, GZ - half, half)
        return wrapped(y + dy, GY), wrapped(z + dz, GZ)

    def copy_of(step, dy):
        ty, tz = target(step, dy)
        k = step * GY + dy
        return pltpu.make_async_remote_copy(
            src_ref=send.at[k],
            dst_ref=recv.at[k],
            send_sem=send_sem.at[k],
            recv_sem=recv_sem.at[k],
            device_id=(x, ty, tz),
            device_id_type=MESH,
        )

    def group(step, carry):
        for dy in range(GY):
            ty, tz = target(step, dy)
            s = ty * GZ + tz
            rows = req[s]
            vx, vy, vz = rows[2:3], rows[3:4], rows[4:5]
            length = jnp.sqrt(vx * vx + vy * vy + vz * vz)
            scale = jnp.maximum(length, 1.0)
            ux, uy, uz = vx / scale, vy / scale, vz / scale
            geo[0:1, :] = rows[0:1]
            geo[1:2, :] = R3 * ux
            geo[2:3, :] = R3 * uy
            geo[3:4, :] = R3 * uz
            geo[4:5, :] = R15 * ux * uy
            geo[5:6, :] = R15 * uy * uz
            geo[6:7, :] = 0.5 * R5 * (2.0 * uz * uz - ux * ux - uy * uy)
            geo[7:8, :] = R15 * ux * uz
            geo[8:9, :] = 0.5 * R15 * (ux * ux - uy * uy)
            geo[9:10, :] = rows[1:2]
            centres = iota((8, CH), 0).astype(F32) * SPACING
            ratio = (length - centres) / SPACING
            geo[16:24, :] = jnp.exp(-(ratio * ratio))
            cols[dy * CAP : (dy + 1) * CAP, 0:32] = jnp.transpose(geo[...])[0:CAP, :]

        def col(k):
            return cols[:, k : k + 1]

        code = col(0)
        live = code >= 0.0
        onehot = jnp.where(code == iota((ROWS, ATOMS), 1).astype(F32), 1.0, 0.0).astype(BF16)
        fetched = dot(onehot, center[...])

        near = col(9)

        def pick(first, count):
            at = iota((ROWS, count), 1).astype(F32) + first
            return jnp.where(near == at, 1.0, 0.0).astype(BF16)

        def gather(i, total):
            rows = halo[pl.ds(i * 3, 3)].reshape(3 * EXPORT, CH)
            first = (i * (3 * EXPORT) + ATOMS).astype(F32)
            return total + dot(pick(first, 3 * EXPORT), rows)

        h_near = lax.fori_loop(0, 9, gather, dot(pick(0.0, ATOMS), center[:, 9 * CH :]))

        def env(m):
            return fetched[:, m * CH : (m + 1) * CH]

        radial = cols[:, 16:24]
        radial_hi = radial.astype(BF16)
        radial_lo = (radial - radial_hi.astype(F32)).astype(BF16)
        pre = dot(env(9).astype(BF16), center_proj[...])
        pre = pre + dot(h_near.astype(BF16), neighbour_proj[...])
        pre = pre + dot(radial_hi, radial_proj[...]) + dot(radial_lo, radial_proj[...])
        hidden = silu(pre).astype(BF16)
        latent = silu(dot(hidden, hidden_proj[...])).astype(BF16)
        mixed = dot(latent, split_proj[...])
        z0, z1, z2 = mixed[:, :CH], mixed[:, CH : 2 * CH], mixed[:, 2 * CH :]
        e0, ex, ey, ez = env(0), env(1), env(2), env(3)
        yx, yy, yz = col(1), col(2), col(3)
        first = (yx * ex + yy * ey + yz * ez) * (1.0 / R3)
        second = col(4) * env(4)
        for m in range(1, 5):
            second = second + col(4 + m) * env(4 + m)
        second = second * (1.0 / R5)
        invariants = jnp.concatenate([z0 * e0, z1 * first, z2 * second], axis=1).astype(BF16)
        update = silu(dot(invariants, scalar_proj[...]))
        out = jnp.where(live, latent.astype(F32) + update, 0.0).astype(BF16)
        a = gain[0:1] * z0
        b = gain[1:2] * z1 * e0
        c = (gain[2:3] * (1.0 / R2)) * z1
        ux = a * ex + b * yx + c * (yy * ez - yz * ey)
        uy = a * ey + b * yy + c * (yz * ex - yx * ez)
        uz = a * ez + b * yz + c * (yx * ey - yy * ex)
        vectors = [jnp.where(live, v, 0.0).astype(BF16) for v in (ux, uy, uz)]
        for dy in range(GY):
            k = step * GY + dy
            cut = slice(dy * CAP, (dy + 1) * CAP)
            send[k, :, 0:LAT] = out[cut]
            for m in range(3):
                send[k, :, LAT + m * CH : LAT + (m + 1) * CH] = vectors[m][cut]

        for dy in range(1, GY):
            copy_of(step, dy).start()

        @pl.when(step < GZ - 1)
        def _():
            copy_of(step, 0).start()

        @pl.when(step == GZ - 1)
        def _():
            recv[step * GY] = send[step * GY]

        pair_energy = jnp.sum(dot_t(w_parts, out), axis=0, keepdims=True)
        e_hi, e_mid, e_lo = parts(jnp.broadcast_to(pair_energy, (8, ROWS)))
        row = iota((8, ROWS), 0)
        e_parts = jnp.where(
            row == 0,
            e_hi.astype(F32),
            jnp.where(row == 1, e_mid.astype(F32), jnp.where(row == 2, e_lo.astype(F32), 0.0)),
        ).astype(BF16)
        energy_ref[...] += dot(e_parts, onehot)
        return carry

    lax.fori_loop(0, GZ, group, 0)

    def landed(step):
        for dy in range(1, GY):
            copy_of(step, dy).wait_recv()

        @pl.when(step < GZ - 1)
        def _():
            copy_of(step, 0).wait_recv()

    def wanted_of(step):
        h = lax.rem(step + 1, GZ)
        half = (h + 1) // 2
        dz = jnp.where(lax.rem(h, 2) == 1, GZ - half, half)
        sz = wrapped(z - dz, GZ)
        lane = iota((8, ROWS), 1)
        wanted = lane
        for dy in range(GY):
            base = (wrapped(y - dy, GY) * GZ + sz) * CAP - dy * CAP
            wanted = jnp.where((lane >= dy * CAP) & (lane < (dy + 1) * CAP), lane + base, wanted)
        return wanted.astype(F32)

    def arrive(turn, carry):
        step = jnp.where(turn == 6, 7, turn)
        landed(step)
        wanted = wanted_of(step)[0:1]
        rows = recv[pl.ds(step * GY, GY)].reshape(ROWS, WIDTH)

        def block(i, c):
            at = pl.ds(pl.multiple_of(i * 256, 256), 256)
            got = dot(jnp.where(slot_col[at, 0:1] == wanted, 1.0, 0.0).astype(BF16), rows)
            acc_ref[at, :] = (acc_ref[at, :].astype(F32) + got).astype(BF16)
            return c

        lax.fori_loop(0, PAIRS // 256, block, 0)
        return carry

    lax.fori_loop(0, GZ - 1, arrive, 0)
    wanted_ref[...] = wanted_of(GZ - 2)
    landed(GZ - 2)
    last_ref[...] = recv[(GZ - 2) * GY : (GZ - 1) * GY].reshape(ROWS, WIDTH)

    def finish(step, carry):
        for dy in range(1, GY):
            copy_of(step, dy).wait_send()

        @pl.when(step < GZ - 1)
        def _():
            copy_of(step, 0).wait_send()

        return carry

    lax.fori_loop(0, GZ, finish, 0)


def last_kernel(slot_ref, wanted_ref, last_ref, acc_ref, parts_ref, latent_ref, vector_ref, energy_ref):
    col = jnp.transpose(slot_ref[...])[:, :1]
    pick = jnp.where(col == wanted_ref[0:1, :], 1.0, 0.0).astype(BF16)
    got = (acc_ref[...].astype(F32) + dot(pick, last_ref[...])).astype(BF16)
    latent_ref[...] = got[:, :LAT]
    for m in range(3):
        vector_ref[m] = got[:, LAT + m * CH : LAT + (m + 1) * CH]
    energy_ref[...] = jnp.sum(parts_ref[...], axis=0, keepdims=True)


def vmem():
    return pl.BlockSpec(memory_space=pltpu.VMEM)


def smem():
    return pl.BlockSpec(memory_space=pltpu.SMEM)


def shaped(shape, dtype):
    return jax.ShapeDtypeStruct(shape, dtype)


def local(
    atom_feat,
    atom_env,
    export_index,
    pair_vec,
    pair_center,
    pair_owner,
    pair_neigh,
    pair_count,
    center_proj,
    neighbour_proj,
    radial_proj,
    hidden_proj,
    split_proj,
    scalar_proj,
    path_gain,
    energy_proj,
):
    acc, last, wanted, slot, energy = pl.pallas_call(
        layer_kernel,
        out_shape=(
            shaped((PAIRS, WIDTH), BF16),
            shaped((ROWS, WIDTH), BF16),
            shaped((8, ROWS), F32),
            shaped((8, PAIRS), F32),
            shaped((8, ATOMS), F32),
        ),
        in_specs=[smem()] + [vmem()] * 5 + [pl.BlockSpec(memory_space=pl.ANY)] * 2 + [vmem()] * 8,
        out_specs=tuple([vmem()] * 5),
        scratch_shapes=[
            pltpu.VMEM((OWN, 8, CH), F32),
            pltpu.VMEM((OWN, 8, CH), F32),
            pltpu.VMEM((27, EXPORT, CH), BF16),
            pltpu.VMEM((ATOMS, 10 * CH), BF16),
            pltpu.VMEM((PAIRS, 8), F32),
            pltpu.VMEM((ROWS, CH), F32),
            pltpu.VMEM((32, CH), F32),
            pltpu.VMEM((OWN, CAP, WIDTH), BF16),
            pltpu.VMEM((OWN, CAP, WIDTH), BF16),
            pltpu.SemaphoreType.DMA((10,)),
            pltpu.SemaphoreType.DMA((31,)),
            pltpu.SemaphoreType.DMA((31,)),
            pltpu.SemaphoreType.DMA((8,)),
            pltpu.SemaphoreType.DMA((8,)),
            pltpu.SemaphoreType.DMA((18,)),
            pltpu.SemaphoreType.DMA((18,)),
            pltpu.SemaphoreType.DMA((OWN,)),
            pltpu.SemaphoreType.DMA((OWN,)),
        ],
        compiler_params=pltpu.CompilerParams(
            collective_id=0, has_side_effects=True, vmem_limit_bytes=60000 * 1024
        ),
    )(
        pair_count,
        pair_owner.reshape(1, PAIRS),
        pair_center.reshape(1, PAIRS),
        pair_neigh.reshape(1, PAIRS),
        pair_vec,
        export_index.reshape(1, EXPORT),
        atom_feat,
        jnp.moveaxis(atom_env, 1, 0),
        center_proj,
        neighbour_proj,
        radial_proj,
        hidden_proj,
        split_proj,
        scalar_proj,
        path_gain,
        energy_proj.reshape(1, LAT),
    )
    size = 512
    latent, vector, atom_energy = pl.pallas_call(
        last_kernel,
        grid=(PAIRS // size,),
        out_shape=(
            shaped((PAIRS, LAT), BF16),
            shaped((3, PAIRS, CH), BF16),
            shaped((1, ATOMS), F32),
        ),
        in_specs=[
            pl.BlockSpec((8, size), lambda i: (0, i)),
            pl.BlockSpec((8, ROWS), lambda i: (0, 0)),
            pl.BlockSpec((ROWS, WIDTH), lambda i: (0, 0)),
            pl.BlockSpec((size, WIDTH), lambda i: (i, 0)),
            pl.BlockSpec((8, ATOMS), lambda i: (0, 0)),
        ],
        out_specs=(
            pl.BlockSpec((size, LAT), lambda i: (i, 0)),
            pl.BlockSpec((3, size, CH), lambda i: (0, i, 0)),
            pl.BlockSpec((1, ATOMS), lambda i: (0, 0)),
        ),
        compiler_params=pltpu.CompilerParams(vmem_limit_bytes=60000 * 1024),
    )(slot, wanted, last, acc, energy)
    return (latent, vector, atom_energy.reshape(ATOMS))


def solution(mesh):
    rows = ("gx", "gy", "gz")
    placed = (
        P(rows, None),
        P(rows, None, None),
        P(rows),
        P(None, rows),
        P(rows),
        P(rows, None),
        P(rows),
        P(rows),
    ) + (P(),) * 8
    return jax.shard_map(
        local,
        mesh=mesh,
        in_specs=placed,
        out_specs=(P(rows, None), P(None, rows, None), P(rows)),
        check_vma=False,
    )
```

```python
import jax
import jax.numpy as jnp
from jax import lax
from jax.experimental import pallas as pl
from jax.experimental.pallas import tpu as pltpu
from jax.sharding import PartitionSpec as P

MESH = pl.DeviceIdType.MESH
F32 = jnp.float32
BF16 = jnp.bfloat16
GX, GY, GZ = 8, 4, 8
OWN = GY * GZ
CAP = 96
PAIRS = 2048
ATOMS = 1024
EXPORT = 256
CH = 128
LAT = 512
WIDTH = LAT + 3 * CH
ROWS = GY * CAP
SPACING = 6.0 / 7.0
R2, R3, R5, R15 = 2.0**0.5, 3.0**0.5, 5.0**0.5, 15.0**0.5

PEERS = [(dy, dz) for dz in range(GZ) for dy in range(GY) if (dy, dz) != (0, 0)]
AROUND = [(oy, oz) for oy in (-1, 0, 1) for oz in (-1, 0, 1) if (oy, oz) != (0, 0)]


def iota(shape, dim):
    return lax.broadcasted_iota(jnp.int32, shape, dim)


def parts(v):
    hi = v.astype(BF16)
    rest = v - hi.astype(F32)
    mid = rest.astype(BF16)
    lo = (rest - mid.astype(F32)).astype(BF16)
    return hi, mid, lo


def dot(a, b):
    return jnp.dot(a, b, preferred_element_type=F32)


def dot_t(a, b):
    return lax.dot_general(a, b, (((1,), (1,)), ((), ())), preferred_element_type=F32)


def wrapped(v, n):
    return lax.rem(v + n, n)


def silu(v):
    return v * jax.nn.sigmoid(v)


def layer_kernel(
    count_ref,
    owner_ref,
    center_ref,
    neigh_ref,
    vec_ref,
    export_ref,
    feat_ref,
    env_ref,
    center_proj,
    neighbour_proj,
    radial_proj,
    hidden_proj,
    split_proj,
    scalar_proj,
    gain_ref,
    energy_proj,
    acc_ref,
    last_ref,
    wanted_ref,
    slot_ref,
    energy_ref,
    ask,
    req,
    halo,
    center,
    slot_col,
    cols,
    geo,
    send,
    recv,
    load_sem,
    req_send,
    req_recv,
    halo_send,
    halo_recv,
    side_send,
    side_recv,
    send_sem,
    recv_sem,
):
    x, y, z = lax.axis_index("gx"), lax.axis_index("gy"), lax.axis_index("gz")
    me = y * GZ + z
    barrier = pltpu.get_barrier_semaphore()
    for dy, dz in PEERS:
        pl.semaphore_signal(
            barrier,
            inc=1,
            device_id=(x, wrapped(y + dy, GY), wrapped(z + dz, GZ)),
            device_id_type=MESH,
        )
    for side in (1, -1):
        pl.semaphore_signal(
            barrier,
            inc=1,
            device_id=(wrapped(x + side, GX), y, z),
            device_id_type=MESH,
        )

    loads = [
        pltpu.make_async_copy(env_ref.at[m], center.at[:, m * CH : (m + 1) * CH], load_sem.at[m])
        for m in range(9)
    ]
    loads.append(pltpu.make_async_copy(feat_ref, center.at[:, 9 * CH :], load_sem.at[9]))
    for c in reversed(loads):
        c.start()

    index8 = jnp.broadcast_to(export_ref[...].astype(F32), (8, EXPORT))
    index_col = jnp.transpose(index8)[:, :1]
    pick = jnp.where(index_col == iota((EXPORT, ATOMS), 1).astype(F32), 1.0, 0.0).astype(BF16)
    loads[9].wait()
    halo[13] = dot(pick, center[:, 9 * CH :]).astype(BF16)

    owner = owner_ref[...]
    member = jnp.where(owner == iota((OWN, PAIRS), 0), 1.0, 0.0)
    member_b = member.astype(BF16)
    block = 256
    before = jnp.where(iota((block, block), 0) < iota((block, block), 1), 1.0, 0.0).astype(BF16)
    running = jnp.zeros((OWN, 1), F32)
    pieces = []
    for b in range(PAIRS // block):
        cut = member_b[:, b * block : (b + 1) * block]
        pieces.append(dot(cut, before) + running)
        running = running + jnp.sum(
            member[:, b * block : (b + 1) * block], axis=1, keepdims=True
        )
    earlier = jnp.concatenate(pieces, axis=1)
    rank = jnp.sum(member * earlier, axis=0, keepdims=True)
    slot_ref[...] = jnp.broadcast_to(owner.astype(F32) * CAP + rank, (8, PAIRS))

    live = iota((1, PAIRS), 1) < count_ref[0]
    code = jnp.where(live, center_ref[...] + 1, 0).astype(F32)
    near = neigh_ref[...].astype(F32)
    field = iota((8, PAIRS), 0)
    values = jnp.where(field == 0, code, jnp.where(field == 1, near, 0.0))
    for m in range(3):
        values = jnp.where(field == 2 + m, vec_ref[m : m + 1, :], values)
    at_rank = jnp.where(rank == iota((CH, PAIRS), 0).astype(F32), 1.0, 0.0).astype(BF16)
    packed = jnp.zeros((OWN * 8, CH), F32)
    for part in parts(values):
        wide = part.astype(F32)
        stacked = jnp.concatenate(
            [jnp.where(owner == o, wide, 0.0) for o in range(OWN)], axis=0
        ).astype(BF16)
        packed = packed + dot_t(stacked, at_rank)
    code_row = jnp.where(iota((8, CH), 0) == 0, 1.0, 0.0)
    for o in range(OWN):
        ask[o] = packed[o * 8 : (o + 1) * 8] - code_row

    pl.semaphore_wait(barrier, len(PEERS) + 2)
    plane, requests, sides = [], [], []
    for k, (oy, oz) in enumerate(AROUND):
        plane.append(
            pltpu.make_async_remote_copy(
                src_ref=halo.at[13],
                dst_ref=halo.at[13 + 3 * oy + oz],
                send_sem=halo_send.at[k],
                recv_sem=halo_recv.at[k],
                device_id=(x, wrapped(y - oy, GY), wrapped(z - oz, GZ)),
                device_id_type=MESH,
            )
        )
    for k, (dy, dz) in enumerate(PEERS):
        ty, tz = wrapped(y + dy, GY), wrapped(z + dz, GZ)
        requests.append(
            pltpu.make_async_remote_copy(
                src_ref=ask.at[ty * GZ + tz],
                dst_ref=req.at[me],
                send_sem=req_send.at[k],
                recv_sem=req_recv.at[k],
                device_id=(x, ty, tz),
                device_id_type=MESH,
            )
        )
    for k, (oy, oz) in enumerate(((0, 0),) + tuple(AROUND)):
        cell = 13 + 3 * oy + oz
        for e, side in enumerate((1, -1)):
            sides.append(
                pltpu.make_async_remote_copy(
                    src_ref=halo.at[cell],
                    dst_ref=halo.at[cell - 9 * side],
                    send_sem=side_send.at[2 * k + e],
                    recv_sem=side_recv.at[2 * k + e],
                    device_id=(wrapped(x + side, GX), y, z),
                    device_id_type=MESH,
                )
            )
    for c in plane + sides[:2] + requests:
        c.start()
    req[me] = ask[me]
    for k, c in enumerate(plane):
        c.wait_recv()
        sides[2 * k + 2].start()
        sides[2 * k + 3].start()
    for c in requests:
        c.wait_recv()
    for c in plane + requests:
        c.wait_send()
    for c in loads[:9]:
        c.wait()

    energy_ref[...] = jnp.zeros_like(energy_ref)
    gain = gain_ref[...]
    weight = jnp.broadcast_to(energy_proj[...], (8, LAT))
    w_hi, w_mid, w_lo = parts(weight)
    row8 = iota((8, LAT), 0)
    w_parts = jnp.where(
        row8 == 0,
        w_hi.astype(F32),
        jnp.where(row8 == 1, w_mid.astype(F32), jnp.where(row8 == 2, w_lo.astype(F32), 0.0)),
    ).astype(BF16)

    slot_col[...] = jnp.transpose(slot_ref[...])
    acc_ref[...] = jnp.zeros_like(acc_ref)

    def target(step, dy):
        h = lax.rem(step + 1, GZ)
        half = (h + 1) // 2
        dz = jnp.where(lax.rem(h, 2) == 1, GZ - half, half)
        return wrapped(y + dy, GY), wrapped(z + dz, GZ)

    def copy_of(step, dy):
        ty, tz = target(step, dy)
        k = step * GY + dy
        return pltpu.make_async_remote_copy(
            src_ref=send.at[k],
            dst_ref=recv.at[k],
            send_sem=send_sem.at[k],
            recv_sem=recv_sem.at[k],
            device_id=(x, ty, tz),
            device_id_type=MESH,
        )

    def group(step, carry):
        for dy in range(GY):
            ty, tz = target(step, dy)
            s = ty * GZ + tz
            rows = req[s]
            vx, vy, vz = rows[2:3], rows[3:4], rows[4:5]
            length = jnp.sqrt(vx * vx + vy * vy + vz * vz)
            scale = jnp.maximum(length, 1.0)
            ux, uy, uz = vx / scale, vy / scale, vz / scale
            geo[0:1, :] = rows[0:1]
            geo[1:2, :] = R3 * ux
            geo[2:3, :] = R3 * uy
            geo[3:4, :] = R3 * uz
            geo[4:5, :] = R15 * ux * uy
            geo[5:6, :] = R15 * uy * uz
            geo[6:7, :] = 0.5 * R5 * (2.0 * uz * uz - ux * ux - uy * uy)
            geo[7:8, :] = R15 * ux * uz
            geo[8:9, :] = 0.5 * R15 * (ux * ux - uy * uy)
            geo[9:10, :] = rows[1:2]
            centres = iota((8, CH), 0).astype(F32) * SPACING
            ratio = (length - centres) / SPACING
            geo[16:24, :] = jnp.exp(-(ratio * ratio))
            cols[dy * CAP : (dy + 1) * CAP, 0:32] = jnp.transpose(geo[...])[0:CAP, :]

        def col(k):
            return cols[:, k : k + 1]

        code = col(0)
        live = code >= 0.0
        onehot = jnp.where(code == iota((ROWS, ATOMS), 1).astype(F32), 1.0, 0.0).astype(BF16)
        fetched = dot(onehot, center[...])

        def env(m):
            return fetched[:, m * CH : (m + 1) * CH]

        radial = cols[:, 16:24]
        radial_hi = radial.astype(BF16)
        radial_lo = (radial - radial_hi.astype(F32)).astype(BF16)
        pre = dot(env(9).astype(BF16), center_proj[...])
        pre = pre + dot(radial_hi, radial_proj[...]) + dot(radial_lo, radial_proj[...])

        @pl.when(step == 0)
        def _():
            for c in sides:
                c.wait()

        near = col(9)

        def pick(first, count):
            at = iota((ROWS, count), 1).astype(F32) + first
            return jnp.where(near == at, 1.0, 0.0).astype(BF16)

        def gather(i, total):
            rows = halo[pl.ds(i * 3, 3)].reshape(3 * EXPORT, CH)
            first = (i * (3 * EXPORT) + ATOMS).astype(F32)
            return total + dot(pick(first, 3 * EXPORT), rows)

        h_near = lax.fori_loop(0, 9, gather, dot(pick(0.0, ATOMS), center[:, 9 * CH :]))
        pre = pre + dot(h_near.astype(BF16), neighbour_proj[...])
        hidden = silu(pre).astype(BF16)
        latent = silu(dot(hidden, hidden_proj[...])).astype(BF16)
        mixed = dot(latent, split_proj[...])
        z0, z1, z2 = mixed[:, :CH], mixed[:, CH : 2 * CH], mixed[:, 2 * CH :]
        e0, ex, ey, ez = env(0), env(1), env(2), env(3)
        yx, yy, yz = col(1), col(2), col(3)
        first = (yx * ex + yy * ey + yz * ez) * (1.0 / R3)
        second = col(4) * env(4)
        for m in range(1, 5):
            second = second + col(4 + m) * env(4 + m)
        second = second * (1.0 / R5)
        invariants = jnp.concatenate([z0 * e0, z1 * first, z2 * second], axis=1).astype(BF16)
        update = silu(dot(invariants, scalar_proj[...]))
        out = jnp.where(live, latent.astype(F32) + update, 0.0).astype(BF16)
        a = gain[0:1] * z0
        b = gain[1:2] * z1 * e0
        c = (gain[2:3] * (1.0 / R2)) * z1
        ux = a * ex + b * yx + c * (yy * ez - yz * ey)
        uy = a * ey + b * yy + c * (yz * ex - yx * ez)
        uz = a * ez + b * yz + c * (yx * ey - yy * ex)
        vectors = [jnp.where(live, v, 0.0).astype(BF16) for v in (ux, uy, uz)]
        for dy in range(GY):
            k = step * GY + dy
            cut = slice(dy * CAP, (dy + 1) * CAP)
            send[k, :, 0:LAT] = out[cut]
            for m in range(3):
                send[k, :, LAT + m * CH : LAT + (m + 1) * CH] = vectors[m][cut]

        for dy in range(1, GY):
            copy_of(step, dy).start()

        @pl.when(step < GZ - 1)
        def _():
            copy_of(step, 0).start()

        @pl.when(step == GZ - 1)
        def _():
            recv[step * GY] = send[step * GY]

        pair_energy = jnp.sum(dot_t(w_parts, out), axis=0, keepdims=True)
        e_hi, e_mid, e_lo = parts(jnp.broadcast_to(pair_energy, (8, ROWS)))
        row = iota((8, ROWS), 0)
        e_parts = jnp.where(
            row == 0,
            e_hi.astype(F32),
            jnp.where(row == 1, e_mid.astype(F32), jnp.where(row == 2, e_lo.astype(F32), 0.0)),
        ).astype(BF16)
        energy_ref[...] += dot(e_parts, onehot)
        return carry

    lax.fori_loop(0, GZ, group, 0)

    def landed(step):
        for dy in range(1, GY):
            copy_of(step, dy).wait_recv()

        @pl.when(step < GZ - 1)
        def _():
            copy_of(step, 0).wait_recv()

    def wanted_of(step):
        h = lax.rem(step + 1, GZ)
        half = (h + 1) // 2
        dz = jnp.where(lax.rem(h, 2) == 1, GZ - half, half)
        sz = wrapped(z - dz, GZ)
        lane = iota((8, ROWS), 1)
        wanted = lane
        for dy in range(GY):
            base = (wrapped(y - dy, GY) * GZ + sz) * CAP - dy * CAP
            wanted = jnp.where((lane >= dy * CAP) & (lane < (dy + 1) * CAP), lane + base, wanted)
        return wanted.astype(F32)

    def arrive(turn, carry):
        step = jnp.where(turn == 6, 7, turn)
        landed(step)
        wanted = wanted_of(step)[0:1]
        rows = recv[pl.ds(step * GY, GY)].reshape(ROWS, WIDTH)

        def block(i, c):
            at = pl.ds(pl.multiple_of(i * 256, 256), 256)
            got = dot(jnp.where(slot_col[at, 0:1] == wanted, 1.0, 0.0).astype(BF16), rows)
            acc_ref[at, :] = (acc_ref[at, :].astype(F32) + got).astype(BF16)
            return c

        lax.fori_loop(0, PAIRS // 256, block, 0)
        return carry

    lax.fori_loop(0, GZ - 1, arrive, 0)
    wanted_ref[...] = wanted_of(GZ - 2)
    landed(GZ - 2)
    last_ref[...] = recv[(GZ - 2) * GY : (GZ - 1) * GY].reshape(ROWS, WIDTH)

    def finish(step, carry):
        for dy in range(1, GY):
            copy_of(step, dy).wait_send()

        @pl.when(step < GZ - 1)
        def _():
            copy_of(step, 0).wait_send()

        return carry

    lax.fori_loop(0, GZ, finish, 0)


def last_kernel(slot_ref, wanted_ref, last_ref, acc_ref, parts_ref, latent_ref, vector_ref, energy_ref):
    col = jnp.transpose(slot_ref[...])[:, :1]
    pick = jnp.where(col == wanted_ref[0:1, :], 1.0, 0.0).astype(BF16)
    got = (acc_ref[...].astype(F32) + dot(pick, last_ref[...])).astype(BF16)
    latent_ref[...] = got[:, :LAT]
    for m in range(3):
        vector_ref[m] = got[:, LAT + m * CH : LAT + (m + 1) * CH]
    energy_ref[...] = jnp.sum(parts_ref[...], axis=0, keepdims=True)


def vmem():
    return pl.BlockSpec(memory_space=pltpu.VMEM)


def smem():
    return pl.BlockSpec(memory_space=pltpu.SMEM)


def shaped(shape, dtype):
    return jax.ShapeDtypeStruct(shape, dtype)


def local(
    atom_feat,
    atom_env,
    export_index,
    pair_vec,
    pair_center,
    pair_owner,
    pair_neigh,
    pair_count,
    center_proj,
    neighbour_proj,
    radial_proj,
    hidden_proj,
    split_proj,
    scalar_proj,
    path_gain,
    energy_proj,
):
    acc, last, wanted, slot, energy = pl.pallas_call(
        layer_kernel,
        out_shape=(
            shaped((PAIRS, WIDTH), BF16),
            shaped((ROWS, WIDTH), BF16),
            shaped((8, ROWS), F32),
            shaped((8, PAIRS), F32),
            shaped((8, ATOMS), F32),
        ),
        in_specs=[smem()] + [vmem()] * 5 + [pl.BlockSpec(memory_space=pl.ANY)] * 2 + [vmem()] * 8,
        out_specs=tuple([vmem()] * 5),
        scratch_shapes=[
            pltpu.VMEM((OWN, 8, CH), F32),
            pltpu.VMEM((OWN, 8, CH), F32),
            pltpu.VMEM((27, EXPORT, CH), BF16),
            pltpu.VMEM((ATOMS, 10 * CH), BF16),
            pltpu.VMEM((PAIRS, 8), F32),
            pltpu.VMEM((ROWS, CH), F32),
            pltpu.VMEM((32, CH), F32),
            pltpu.VMEM((OWN, CAP, WIDTH), BF16),
            pltpu.VMEM((OWN, CAP, WIDTH), BF16),
            pltpu.SemaphoreType.DMA((10,)),
            pltpu.SemaphoreType.DMA((31,)),
            pltpu.SemaphoreType.DMA((31,)),
            pltpu.SemaphoreType.DMA((8,)),
            pltpu.SemaphoreType.DMA((8,)),
            pltpu.SemaphoreType.DMA((18,)),
            pltpu.SemaphoreType.DMA((18,)),
            pltpu.SemaphoreType.DMA((OWN,)),
            pltpu.SemaphoreType.DMA((OWN,)),
        ],
        compiler_params=pltpu.CompilerParams(
            collective_id=0, has_side_effects=True, vmem_limit_bytes=60000 * 1024
        ),
    )(
        pair_count,
        pair_owner.reshape(1, PAIRS),
        pair_center.reshape(1, PAIRS),
        pair_neigh.reshape(1, PAIRS),
        pair_vec,
        export_index.reshape(1, EXPORT),
        atom_feat,
        jnp.moveaxis(atom_env, 1, 0),
        center_proj,
        neighbour_proj,
        radial_proj,
        hidden_proj,
        split_proj,
        scalar_proj,
        path_gain,
        energy_proj.reshape(1, LAT),
    )
    size = 1024
    latent, vector, atom_energy = pl.pallas_call(
        last_kernel,
        grid=(PAIRS // size,),
        out_shape=(
            shaped((PAIRS, LAT), BF16),
            shaped((3, PAIRS, CH), BF16),
            shaped((1, ATOMS), F32),
        ),
        in_specs=[
            pl.BlockSpec((8, size), lambda i: (0, i)),
            pl.BlockSpec((8, ROWS), lambda i: (0, 0)),
            pl.BlockSpec((ROWS, WIDTH), lambda i: (0, 0)),
            pl.BlockSpec((size, WIDTH), lambda i: (i, 0)),
            pl.BlockSpec((8, ATOMS), lambda i: (0, 0)),
        ],
        out_specs=(
            pl.BlockSpec((size, LAT), lambda i: (i, 0)),
            pl.BlockSpec((3, size, CH), lambda i: (0, i, 0)),
            pl.BlockSpec((1, ATOMS), lambda i: (0, 0)),
        ),
        compiler_params=pltpu.CompilerParams(vmem_limit_bytes=60000 * 1024),
    )(slot, wanted, last, acc, energy)
    return (latent, vector, atom_energy.reshape(ATOMS))


def solution(mesh):
    rows = ("gx", "gy", "gz")
    placed = (
        P(rows, None),
        P(rows, None, None),
        P(rows),
        P(None, rows),
        P(rows),
        P(rows, None),
        P(rows),
        P(rows),
    ) + (P(),) * 8
    return jax.shard_map(
        local,
        mesh=mesh,
        in_specs=placed,
        out_specs=(P(rows, None), P(None, rows, None), P(rows)),
        check_vma=False,
    )
```
